32 devices in a mesh: dp: 2 (over x), tp: 4 (over z), cp: 4 (over y, core).
Axes of the slice: x: 2, y: 2, z: 4, core: 2. Of those that a mesh axis runs over, the one named last changes fastest.
Arguments:
- x: bfloat16 [4, 512, 12288], P('dp', 'cp'), parts along dimension 0
- prefix_len: int32 [4], P('dp'), parts along dimension 0
- valid_len: int32 [4], P('dp'), parts along dimension 0
- w_qkv: bfloat16 [12288, 3, 96, 128], P(None, None, 'tp')
- b_qkv: bfloat16 [3, 96, 128], P(None, 'tp')
- w_out: bfloat16 [96, 128, 12288], P('tp')
- b_out: bfloat16 [12288], replicated
- ln_gamma: bfloat16 [12288], replicated
- ln_beta: bfloat16 [12288], replicated
Outputs:
- output 1: bfloat16 [4, 512, 12288], P('dp', 'cp'), parts along dimension 0
- output 2: bfloat16 [4, 512, 96, 128], P('dp', 'cp', 'tp'), parts along dimension 0
- output 3: bfloat16 [4, 512, 96, 128], P('dp', 'cp', 'tp'), parts along dimension 0
There are 2 independent parts. The reference program is written for one: setup_inputs(seed, part) draws one part's arguments, and reference() takes and returns one part's arrays. A program takes and returns all parts, laid end to end along the dimension named above; an argument that names none is the same for every part.
All inputs are finite; a program needn't handle non-finite values.
Results may differ from the reference program's by a relative error of at most 0.0100757.
Values are sent between devices in bfloat16 or wider.
A program may use at most 1.25 GiB of HBM per device.

```python
import math
import jax
import jax.numpy as jnp
from jax import lax

BATCH_ROWS = 2
SEQ_LEN = 512
D_MODEL = 12288
N_HEADS = 96
HEAD_DIM = 128

ALPHA = math.sqrt(140.0)
ROPE_BASE = 10000.0
LN_EPS = 1e-5


def setup_inputs(seed: int = 0, part: int = 0) -> dict:
    part_key = jax.random.fold_in(jax.random.key(seed), part)
    part_keys = jax.random.split(part_key, 3)
    weight_keys = jax.random.split(jax.random.key(seed + 1), 6)
    x = jax.random.normal(part_keys[0], (BATCH_ROWS, SEQ_LEN, D_MODEL), jnp.float32)
    valid_len = jax.random.randint(part_keys[1], (BATCH_ROWS,), (3 * SEQ_LEN) // 4, SEQ_LEN + 1, dtype=jnp.int32)
    prefix_len = jax.random.randint(part_keys[2], (BATCH_ROWS,), SEQ_LEN // 2, valid_len + 1, dtype=jnp.int32)
    w_scale = D_MODEL ** -0.5
    out_scale = 0.5 * ALPHA * (SEQ_LEN / D_MODEL) ** 0.5
    w_qkv = jax.random.normal(weight_keys[0], (D_MODEL, 3, N_HEADS, HEAD_DIM), jnp.float32) * w_scale
    b_qkv = jax.random.normal(weight_keys[1], (3, N_HEADS, HEAD_DIM), jnp.float32) * SEQ_LEN ** -0.5
    w_out = jax.random.normal(weight_keys[2], (N_HEADS, HEAD_DIM, D_MODEL), jnp.float32) * out_scale
    b_out = jax.random.normal(weight_keys[3], (D_MODEL,), jnp.float32) * (0.5 * ALPHA)
    ln_gamma = 1.0 + 0.3 * jax.random.normal(weight_keys[4], (D_MODEL,), jnp.float32)
    ln_beta = 0.2 * jax.random.normal(weight_keys[5], (D_MODEL,), jnp.float32)
    return {
        "x": x.astype(jnp.bfloat16),
        "prefix_len": prefix_len,
        "valid_len": valid_len,
        "w_qkv": w_qkv.astype(jnp.bfloat16),
        "b_qkv": b_qkv.astype(jnp.bfloat16),
        "w_out": w_out.astype(jnp.bfloat16),
        "b_out": b_out.astype(jnp.bfloat16),
        "ln_gamma": ln_gamma.astype(jnp.bfloat16),
        "ln_beta": ln_beta.astype(jnp.bfloat16),
    }


def rope_tables(length):
    positions = jnp.arange(length).astype(jnp.float32)
    inv_freq = ROPE_BASE ** (-jnp.arange(0, HEAD_DIM, 2).astype(jnp.float32) / HEAD_DIM)
    angles = positions[:, None] * inv_freq[None, :]
    angles = jnp.concatenate([angles, angles], axis=-1)
    return jnp.cos(angles), jnp.sin(angles)


def apply_rope(tensor, cos_tab, sin_tab):
    half_dim = HEAD_DIM // 2
    rotated = jnp.concatenate([-tensor[..., half_dim:], tensor[..., :half_dim]], axis=-1)
    return tensor * cos_tab[None, :, None, :] + rotated * sin_tab[None, :, None, :]


def by_head(tensor):
    return tensor.transpose(0, 2, 1, 3).reshape(BATCH_ROWS * N_HEADS, SEQ_LEN, HEAD_DIM)


def reference(x, prefix_len, valid_len, w_qkv, b_qkv, w_out, b_out, ln_gamma, ln_beta):
    x_rows = x.reshape(BATCH_ROWS * SEQ_LEN, D_MODEL)
    qkv_all = jnp.dot(x_rows, w_qkv.reshape(D_MODEL, 3 * N_HEADS * HEAD_DIM), preferred_element_type=jnp.float32)
    qkv_all = qkv_all.reshape(BATCH_ROWS, SEQ_LEN, 3, N_HEADS, HEAD_DIM) + b_qkv.astype(jnp.float32)
    cos_tab, sin_tab = rope_tables(SEQ_LEN)
    queries = apply_rope(qkv_all[:, :, 0], cos_tab, sin_tab).astype(jnp.bfloat16)
    keys = apply_rope(qkv_all[:, :, 1], cos_tab, sin_tab).astype(jnp.bfloat16)
    values = qkv_all[:, :, 2].astype(jnp.bfloat16)
    prefix_rep = jnp.repeat(prefix_len, N_HEADS)
    valid_rep = jnp.repeat(valid_len, N_HEADS)
    positions = jnp.arange(SEQ_LEN)
    score_scale = HEAD_DIM ** -0.5

    def head_attention(head_item):
        q_one, k_one, v_one, prefix_one, valid_one = head_item
        scores = jnp.dot(q_one, k_one.T, preferred_element_type=jnp.float32) * score_scale
        key_pos = positions[None, :]
        allowed = (key_pos < valid_one) & ((key_pos < prefix_one) | (key_pos <= positions[:, None]))
        scores = jnp.where(allowed, scores, -1e30)
        row_max = jnp.max(scores, axis=-1, keepdims=True)
        weights = jnp.where(allowed, jnp.exp(scores - row_max), 0.0)
        row_sum = jnp.sum(weights, axis=-1, keepdims=True)
        mixed_sum = jnp.dot(weights.astype(jnp.bfloat16), v_one, preferred_element_type=jnp.float32)
        return (mixed_sum / row_sum).astype(jnp.bfloat16)

    attn_out = lax.map(head_attention, (by_head(queries), by_head(keys), by_head(values), prefix_rep, valid_rep))
    attn_out = attn_out.reshape(BATCH_ROWS, N_HEADS, SEQ_LEN, HEAD_DIM).transpose(0, 2, 1, 3)
    attn_out = attn_out.reshape(BATCH_ROWS * SEQ_LEN, N_HEADS * HEAD_DIM)
    proj_out = jnp.dot(attn_out, w_out.reshape(N_HEADS * HEAD_DIM, D_MODEL), preferred_element_type=jnp.float32)
    residual = ALPHA * x_rows.astype(jnp.float32) + proj_out + b_out.astype(jnp.float32)
    row_mean = jnp.mean(residual, axis=-1, keepdims=True)
    centered = residual - row_mean
    row_var = jnp.mean(centered * centered, axis=-1, keepdims=True)
    normed = centered * lax.rsqrt(row_var + LN_EPS) * ln_gamma.astype(jnp.float32) + ln_beta.astype(jnp.float32)
    out = normed.astype(jnp.bfloat16).reshape(BATCH_ROWS, SEQ_LEN, D_MODEL)
    return out, keys, values
```

```python
import functools
import math
import jax
import jax.numpy as jnp
from jax import lax
from jax.experimental import pallas as pl
from jax.experimental.pallas import tpu as pltpu
from jax.sharding import PartitionSpec as P

ALPHA = math.sqrt(140.0)
ROPE_BASE = 10000.0
LN_EPS = 1e-5
HEAD_GROUP = 4
VMEM_LIMIT = 60 * 2**20


def rope_tables(positions, head_dim):
    inv_freq = ROPE_BASE ** (-jnp.arange(0, head_dim, 2).astype(jnp.float32) / head_dim)
    angles = positions.astype(jnp.float32)[:, None] * inv_freq[None, :]
    cos_half, sin_half = jnp.cos(angles), jnp.sin(angles)
    return jnp.concatenate([cos_half, cos_half], axis=-1), jnp.concatenate([-sin_half, sin_half], axis=-1)


def project_kernel(rope, core_ref, x_own_ref, x_other_ref, w_ref, bias_ref, cos_ref, sin_ref, o_ref, acc, wide):
    step = pl.program_id(0)
    depth, groups = w_ref.shape[0], w_ref.shape[2]
    head_dim = w_ref.shape[4]

    @pl.when(step == 0)
    def _():
        acc[...] = jnp.zeros_like(acc)

    x_rows = jnp.concatenate([x_own_ref[...], x_other_ref[...]], axis=0)
    for group in range(groups):
        wide[group] = w_ref[:, 0, group].astype(jnp.float32).reshape(depth * HEAD_GROUP, head_dim)
    for head in range(0, groups * HEAD_GROUP, 2):
        group, lane = divmod(head, HEAD_GROUP)
        first = wide[group, pl.ds(lane, depth, stride=HEAD_GROUP), :].astype(jnp.bfloat16)
        second = wide[group, pl.ds(lane + 1, depth, stride=HEAD_GROUP), :].astype(jnp.bfloat16)
        cols = slice(head * head_dim, (head + 2) * head_dim)
        acc[:, cols] += jnp.dot(x_rows, jnp.concatenate([first, second], axis=1), preferred_element_type=jnp.float32)

    @pl.when(step == pl.num_programs(0) - 1)
    def _():
        for head in range(groups * HEAD_GROUP):
            cols = slice(head * head_dim, (head + 1) * head_dim)
            value = acc[:, cols] + bias_ref[0:1, cols]
            if rope:
                value = value * cos_ref[...] + pltpu.roll(value, head_dim // 2, 1) * sin_ref[...]
            o_ref[:, cols] = value.astype(jnp.bfloat16)


def project(which, core, x_own, x_other, w_grouped, bias, cos_tab, sin_tab, depth):
    rows, d_model = x_own.shape
    groups = w_grouped.shape[2] // 2
    head_dim = w_grouped.shape[4]
    width = groups * HEAD_GROUP * head_dim
    return pl.pallas_call(
        functools.partial(project_kernel, which != 2),
        grid_spec=pltpu.PrefetchScalarGridSpec(
            num_scalar_prefetch=1,
            grid=(d_model // depth,),
            in_specs=[
                pl.BlockSpec((rows, depth), lambda k, core: (0, k)),
                pl.BlockSpec((rows, depth), lambda k, core: (0, k)),
                pl.BlockSpec((depth, 1, groups, HEAD_GROUP, head_dim), lambda k, core: (k, which, core[0], 0, 0)),
                pl.BlockSpec((8, width), lambda k, core: (0, core[0])),
                pl.BlockSpec((2 * rows, head_dim), lambda k, core: (0, 0)),
                pl.BlockSpec((2 * rows, head_dim), lambda k, core: (0, 0)),
            ],
            out_specs=pl.BlockSpec((2 * rows, width), lambda k, core: (0, 0)),
            scratch_shapes=[
                pltpu.VMEM((2 * rows, width), jnp.float32),
                pltpu.VMEM((groups, depth * HEAD_GROUP, head_dim), jnp.float32),
            ],
        ),
        out_shape=jax.ShapeDtypeStruct((2 * rows, width), jnp.bfloat16),
        compiler_params=pltpu.CompilerParams(vmem_limit_bytes=VMEM_LIMIT),
        cost_estimate=pl.CostEstimate(
            flops=4 * rows * d_model * width, bytes_accessed=2 * d_model * (width + 2 * rows), transcendentals=0
        ),
        name=("project_q", "project_k", "project_v")[which],
    )(core, x_own, x_other, w_grouped, bias, cos_tab, sin_tab)


def attend_kernel(batch, info_ref, q_ref, k_near_ref, v_near_ref, k_far_ref, v_far_ref, o_ref):
    piece = q_ref.shape[0] // (2 * batch)
    scale = q_ref.shape[1] ** -0.5

    def pick(ref, half, seq):
        start = (half * batch + seq) * piece
        return ref[start : start + piece, :]

    row_iota = lax.broadcasted_iota(jnp.int32, (piece, 1), 0)
    lane_iota = lax.broadcasted_iota(jnp.int32, (1, piece), 1)
    q_pos = jnp.concatenate([row_iota + info_ref[i] * piece for i in range(2)], axis=0)
    k_pos = jnp.concatenate([lane_iota + info_ref[i] * piece for i in range(4)], axis=1)
    for seq in range(batch):
        prefix, valid = info_ref[4 + seq], info_ref[4 + batch + seq]
        q = jnp.concatenate([pick(q_ref, 0, seq), pick(q_ref, 1, seq)], axis=0)
        k = jnp.concatenate([pick(r, i, seq) for r in (k_near_ref, k_far_ref) for i in range(2)], axis=0)
        v = jnp.concatenate([pick(r, i, seq) for r in (v_near_ref, v_far_ref) for i in range(2)], axis=0)
        scores = lax.dot_general(q, k, (((1,), (1,)), ((), ())), preferred_element_type=jnp.float32) * scale
        limit = jnp.minimum(jnp.maximum(q_pos + 1, prefix), valid)
        allowed = k_pos < limit
        scores = jnp.where(allowed, scores, -1e30)
        row_max = jnp.max(scores, axis=-1, keepdims=True)
        weights = jnp.where(allowed, jnp.exp(scores - row_max), 0.0)
        row_sum = jnp.sum(weights, axis=-1, keepdims=True)
        mixed = jnp.dot(weights.astype(jnp.bfloat16), v, preferred_element_type=jnp.float32)
        mixed = (mixed / row_sum).astype(jnp.bfloat16)
        for half in range(2):
            start = (half * batch + seq) * piece
            o_ref[start : start + piece, :] = mixed[half * piece : (half + 1) * piece, :]


def attend(info, q, k_near, v_near, k_far, v_far, batch, head_dim):
    rows, width = q.shape
    heads = width // head_dim
    spec = pl.BlockSpec((rows, head_dim), lambda h, info: (0, h))
    return pl.pallas_call(
        functools.partial(attend_kernel, batch),
        grid_spec=pltpu.PrefetchScalarGridSpec(
            num_scalar_prefetch=1, grid=(heads,), in_specs=[spec] * 5, out_specs=spec
        ),
        out_shape=jax.ShapeDtypeStruct((rows, width), jnp.bfloat16),
        compiler_params=pltpu.CompilerParams(vmem_limit_bytes=VMEM_LIMIT),
        cost_estimate=pl.CostEstimate(
            flops=8 * rows * rows * width // batch, bytes_accessed=12 * rows * width, transcendentals=2 * rows * rows * heads // batch
        ),
        name="attend",
    )(info, q, k_near, v_near, k_far, v_far)


def post_norm(x_rows, head_sum, b_out, ln_gamma, ln_beta):
    residual = ALPHA * x_rows.astype(jnp.float32) + head_sum.astype(jnp.float32) + b_out.astype(jnp.float32)
    row_mean = jnp.mean(residual, axis=-1, keepdims=True)
    centered = residual - row_mean
    row_var = jnp.mean(centered * centered, axis=-1, keepdims=True)
    normed = centered * lax.rsqrt(row_var + LN_EPS)
    return (normed * ln_gamma.astype(jnp.float32) + ln_beta.astype(jnp.float32)).astype(jnp.bfloat16)


def solution(mesh):
    cp_size = mesh.shape["cp"]
    swap_core = [(i, i ^ 1) for i in range(cp_size)]
    swap_chip = [(i, i ^ 2) for i in range(cp_size)]

    def device_body(x_loc, prefix_len, valid_len, w_qkv, b_qkv, w_out, b_out, ln_gamma, ln_beta):
        batch, piece, d_model = x_loc.shape
        _, _, heads, head_dim = w_qkv.shape
        rows, half_width = batch * piece, heads * head_dim // 2
        depth = min(512, d_model)
        cp_index = lax.axis_index("cp")
        core_index = lax.rem(cp_index, 2)
        core = core_index.astype(jnp.int32).reshape(1)
        near, far = cp_index ^ 1, cp_index ^ 2
        x_own = x_loc.reshape(rows, d_model)
        x_other = lax.ppermute(x_own, "cp", swap_core)
        w_grouped = w_qkv.reshape(d_model, 3, heads // HEAD_GROUP, HEAD_GROUP, head_dim)
        bias = b_qkv.reshape(3, heads * head_dim).astype(jnp.float32)
        spread = jnp.arange(piece)
        positions = jnp.concatenate([cp_index * piece + spread] * batch + [near * piece + spread] * batch)
        cos_tab, sin_tab = rope_tables(positions, head_dim)

        def run(which, after):
            bias_row = jnp.broadcast_to(bias[which][None], (8, heads * head_dim))
            if after is not None:
                bias_row, _ = lax.optimization_barrier((bias_row, after))
            return project(which, core, x_own, x_other, w_grouped, bias_row, cos_tab, sin_tab, depth)

        def gather_heads(own, received):
            low = jnp.where(core_index == 0, own, received)
            high = jnp.where(core_index == 0, received, own)
            return jnp.concatenate([low, high], axis=1)

        keys = run(1, None)
        keys_far = lax.ppermute(keys, "cp", swap_chip)
        keys_back = lax.ppermute(keys[rows:], "cp", swap_core)
        values = run(2, keys)
        values_far = lax.ppermute(values, "cp", swap_chip)
        values_back = lax.ppermute(values[rows:], "cp", swap_core)
        queries = run(0, values)
        k_cache = gather_heads(keys[:rows], keys_back).reshape(batch, piece, heads, head_dim)
        v_cache = gather_heads(values[:rows], values_back).reshape(batch, piece, heads, head_dim)

        info = jnp.concatenate([jnp.stack([cp_index, near, far, far ^ 1]).astype(jnp.int32), prefix_len, valid_len])
        mixed = attend(info, queries, keys, values, keys_far, values_far, batch, head_dim)
        mixed_back = lax.ppermute(mixed[rows:], "cp", swap_core)
        attn_out = gather_heads(mixed[:rows], mixed_back)
        head_part = jnp.dot(attn_out, w_out.reshape(2 * half_width, d_model), preferred_element_type=jnp.float32)
        head_sum = lax.psum(head_part.astype(jnp.bfloat16).reshape(x_loc.shape), "tp")
        return post_norm(x_loc, head_sum, b_out, ln_gamma, ln_beta), k_cache, v_cache

    return jax.shard_map(
        device_body,
        mesh=mesh,
        in_specs=(
            P("dp", "cp", None),
            P("dp"),
            P("dp"),
            P(None, None, "tp", None),
            P(None, "tp", None),
            P("tp", None, None),
            P(None),
            P(None),
            P(None),
        ),
        out_specs=(P("dp", "cp", None), P("dp", "cp", "tp", None), P("dp", "cp", "tp", None)),
        check_vma=False,
    )
```

```python
import functools
import math
import jax
import jax.numpy as jnp
from jax import lax
from jax.experimental import pallas as pl
from jax.experimental.pallas import tpu as pltpu
from jax.sharding import PartitionSpec as P

ALPHA = math.sqrt(140.0)
ROPE_BASE = 10000.0
LN_EPS = 1e-5
HEAD_GROUP = 4
VMEM_LIMIT = 60 * 2**20


def rope_tables(positions, head_dim):
    inv_freq = ROPE_BASE ** (-jnp.arange(0, head_dim, 2).astype(jnp.float32) / head_dim)
    angles = positions.astype(jnp.float32)[:, None] * inv_freq[None, :]
    cos_half, sin_half = jnp.cos(angles), jnp.sin(angles)
    return jnp.concatenate([cos_half, cos_half], axis=-1), jnp.concatenate([-sin_half, sin_half], axis=-1)


def project_kernel(rope, core_ref, x_own_ref, x_other_ref, w_ref, bias_ref, cos_ref, sin_ref, o_ref, acc, wide):
    step = pl.program_id(0)
    depth, groups = w_ref.shape[0], w_ref.shape[2]
    head_dim = w_ref.shape[4]

    @pl.when(step == 0)
    def _():
        acc[...] = jnp.zeros_like(acc)

    x_rows = jnp.concatenate([x_own_ref[...], x_other_ref[...]], axis=0)
    for group in range(groups):
        wide[group] = w_ref[:, 0, group].astype(jnp.float32).reshape(depth * HEAD_GROUP, head_dim)
    for head in range(0, groups * HEAD_GROUP, 2):
        group, lane = divmod(head, HEAD_GROUP)
        first = wide[group, pl.ds(lane, depth, stride=HEAD_GROUP), :].astype(jnp.bfloat16)
        second = wide[group, pl.ds(lane + 1, depth, stride=HEAD_GROUP), :].astype(jnp.bfloat16)
        cols = slice(head * head_dim, (head + 2) * head_dim)
        acc[:, cols] += jnp.dot(x_rows, jnp.concatenate([first, second], axis=1), preferred_element_type=jnp.float32)

    @pl.when(step == pl.num_programs(0) - 1)
    def _():
        for head in range(groups * HEAD_GROUP):
            cols = slice(head * head_dim, (head + 1) * head_dim)
            value = acc[:, cols] + bias_ref[0:1, cols]
            if rope:
                value = value * cos_ref[...] + pltpu.roll(value, head_dim // 2, 1) * sin_ref[...]
            o_ref[:, cols] = value.astype(jnp.bfloat16)


def project(which, core, x_own, x_other, w_grouped, bias, cos_tab, sin_tab, depth):
    rows, d_model = x_own.shape
    groups = w_grouped.shape[2] // 2
    head_dim = w_grouped.shape[4]
    width = groups * HEAD_GROUP * head_dim
    return pl.pallas_call(
        functools.partial(project_kernel, which != 2),
        grid_spec=pltpu.PrefetchScalarGridSpec(
            num_scalar_prefetch=1,
            grid=(d_model // depth,),
            in_specs=[
                pl.BlockSpec((rows, depth), lambda k, core: (0, k)),
                pl.BlockSpec((rows, depth), lambda k, core: (0, k)),
                pl.BlockSpec((depth, 1, groups, HEAD_GROUP, head_dim), lambda k, core: (k, which, core[0], 0, 0)),
                pl.BlockSpec((8, width), lambda k, core: (0, core[0])),
                pl.BlockSpec((2 * rows, head_dim), lambda k, core: (0, 0)),
                pl.BlockSpec((2 * rows, head_dim), lambda k, core: (0, 0)),
            ],
            out_specs=pl.BlockSpec((2 * rows, width), lambda k, core: (0, 0)),
            scratch_shapes=[
                pltpu.VMEM((2 * rows, width), jnp.float32),
                pltpu.VMEM((groups, depth * HEAD_GROUP, head_dim), jnp.float32),
            ],
        ),
        out_shape=jax.ShapeDtypeStruct((2 * rows, width), jnp.bfloat16),
        compiler_params=pltpu.CompilerParams(vmem_limit_bytes=VMEM_LIMIT),
        cost_estimate=pl.CostEstimate(
            flops=4 * rows * d_model * width, bytes_accessed=2 * d_model * (width + 2 * rows), transcendentals=0
        ),
        name=("project_q", "project_k", "project_v")[which],
    )(core, x_own, x_other, w_grouped, bias, cos_tab, sin_tab)


def attend_kernel(batch, info_ref, q_ref, k_near_ref, v_near_ref, k_far_ref, v_far_ref, o_ref):
    piece = q_ref.shape[0] // (2 * batch)
    scale = q_ref.shape[1] ** -0.5

    def pick(ref, half, seq):
        start = (half * batch + seq) * piece
        return ref[start : start + piece, :]

    row_iota = lax.broadcasted_iota(jnp.int32, (piece, 1), 0)
    lane_iota = lax.broadcasted_iota(jnp.int32, (1, piece), 1)
    q_pos = jnp.concatenate([row_iota + info_ref[i] * piece for i in range(2)], axis=0)
    k_pos = jnp.concatenate([lane_iota + info_ref[i] * piece for i in range(4)], axis=1)
    for seq in range(batch):
        prefix, valid = info_ref[4 + seq], info_ref[4 + batch + seq]
        q = jnp.concatenate([pick(q_ref, 0, seq), pick(q_ref, 1, seq)], axis=0)
        k = jnp.concatenate([pick(r, i, seq) for r in (k_near_ref, k_far_ref) for i in range(2)], axis=0)
        v = jnp.concatenate([pick(r, i, seq) for r in (v_near_ref, v_far_ref) for i in range(2)], axis=0)
        scores = lax.dot_general(q, k, (((1,), (1,)), ((), ())), preferred_element_type=jnp.float32) * scale
        limit = jnp.minimum(jnp.maximum(q_pos + 1, prefix), valid)
        allowed = k_pos < limit
        scores = jnp.where(allowed, scores, -1e30)
        row_max = jnp.max(scores, axis=-1, keepdims=True)
        weights = jnp.where(allowed, jnp.exp(scores - row_max), 0.0)
        row_sum = jnp.sum(weights, axis=-1, keepdims=True)
        mixed = jnp.dot(weights.astype(jnp.bfloat16), v, preferred_element_type=jnp.float32)
        mixed = (mixed / row_sum).astype(jnp.bfloat16)
        for half in range(2):
            start = (half * batch + seq) * piece
            o_ref[start : start + piece, :] = mixed[half * piece : (half + 1) * piece, :]


def attend(info, q, k_near, v_near, k_far, v_far, batch, head_dim):
    rows, width = q.shape
    heads = width // head_dim
    spec = pl.BlockSpec((rows, head_dim), lambda h, info: (0, h))
    return pl.pallas_call(
        functools.partial(attend_kernel, batch),
        grid_spec=pltpu.PrefetchScalarGridSpec(
            num_scalar_prefetch=1, grid=(heads,), in_specs=[spec] * 5, out_specs=spec
        ),
        out_shape=jax.ShapeDtypeStruct((rows, width), jnp.bfloat16),
        compiler_params=pltpu.CompilerParams(vmem_limit_bytes=VMEM_LIMIT),
        cost_estimate=pl.CostEstimate(
            flops=8 * rows * rows * width // batch, bytes_accessed=12 * rows * width, transcendentals=2 * rows * rows * heads // batch
        ),
        name="attend",
    )(info, q, k_near, v_near, k_far, v_far)


def tail_kernel(
    size, lag, a_ref, w_ref, x_ref, b_ref, gamma_ref, beta_ref, out_ref,
    part, w_buf, x_buf, up_out, up_in, up_fin, down_out, down_in, down_fin,
    w_sem, x_sem, sum_send, sum_recv, fin_send, fin_recv, out_sem,
):
    tiles, rows, width = part.shape
    half = rows // 2
    me = lax.axis_index("tp")
    last = size - 1
    barrier = pltpu.get_barrier_semaphore()

    @pl.when(me > 0)
    def _():
        pl.semaphore_signal(barrier, inc=1, device_id={"tp": me - 1}, device_id_type=pl.DeviceIdType.MESH)

    @pl.when(me < last)
    def _():
        pl.semaphore_signal(barrier, inc=1, device_id={"tp": me + 1}, device_id_type=pl.DeviceIdType.MESH)

    pl.semaphore_wait(barrier, jnp.minimum(me, 1) + jnp.minimum(last - me, 1))

    def fetch(tile):
        slot = lax.rem(tile, 2)
        cols = pl.ds(pl.multiple_of(tile * width, width), width)
        return pltpu.make_async_copy(w_ref.at[:, cols], w_buf.at[slot], w_sem.at[slot])

    def send(flow, src, dst, send_sem, recv_sem, tile, peer):
        return pltpu.make_async_remote_copy(
            src_ref=src.at[tile],
            dst_ref=dst.at[tile],
            send_sem=send_sem.at[flow, tile],
            recv_sem=recv_sem.at[flow, tile],
            device_id={"tp": peer},
            device_id_type=pl.DeviceIdType.MESH,
        )

    fetch(0).start()
    x_copy = pltpu.make_async_copy(x_ref, x_buf, x_sem)
    x_copy.start()
    flows = (
        (0, 0, me, me + 1, me - 1, up_out, up_in, up_fin),
        (1, half, last - me, me - 1, me + 1, down_out, down_in, down_fin),
    )

    def sum_step(step, carry):
        @pl.when(step < tiles)
        def _():
            fetch(step).wait()

            @pl.when(step + 1 < tiles)
            def _():
                fetch(step + 1).start()

            part[step] = jnp.dot(a_ref[...], w_buf[lax.rem(step, 2)], preferred_element_type=jnp.float32)

        for flow, base, place, ahead, _, outgoing, incoming, _ in flows:
            tile = step - lag * place

            @pl.when((tile >= 0) & (tile < tiles))
            def _():
                @pl.when(place > 0)
                def _():
                    send(flow, outgoing, incoming, sum_send, sum_recv, tile, ahead).wait_recv()
                    part[tile, base : base + half] += incoming[tile].astype(jnp.float32)

                @pl.when(place < last)
                def _():
                    outgoing[tile] = part[tile, base : base + half].astype(jnp.bfloat16)
                    send(flow, outgoing, incoming, sum_send, sum_recv, tile, ahead).start()

        return carry

    lax.fori_loop(0, tiles + lag * last, sum_step, 0)
    x_copy.wait()

    for flow, base, place, ahead, back, outgoing, incoming, final in flows:
        def norm_tiles(base=base):
            def residual_step(tile, total):
                cols = pl.ds(pl.multiple_of(tile * width, width), width)
                value = part[tile, base : base + half] + ALPHA * x_buf[base : base + half, cols].astype(jnp.float32)
                value = value + b_ref[0:1, cols]
                part[tile, base : base + half] = value
                for i in range(width // 128):
                    total = total + value[:, i * 128 : (i + 1) * 128]
                return total

            zero = jnp.zeros((half, 128), jnp.float32)
            count = tiles * width
            mean = jnp.sum(lax.fori_loop(0, tiles, residual_step, zero), axis=-1, keepdims=True) / count

            def spread_step(tile, total):
                value = part[tile, base : base + half] - mean
                part[tile, base : base + half] = value
                for i in range(width // 128):
                    total = total + value[:, i * 128 : (i + 1) * 128] * value[:, i * 128 : (i + 1) * 128]
                return total

            spread = jnp.sum(lax.fori_loop(0, tiles, spread_step, zero), axis=-1, keepdims=True) / count
            return lax.rsqrt(spread + LN_EPS)

        @pl.when(place == last)
        def _():
            inverse = norm_tiles()

            def write_step(tile, carry):
                cols = pl.ds(pl.multiple_of(tile * width, width), width)
                value = part[tile, base : base + half] * inverse * gamma_ref[0:1, cols] + beta_ref[0:1, cols]
                final[tile] = value.astype(jnp.bfloat16)
                send(flow, final, final, fin_send, fin_recv, tile, back).start()
                return carry

            lax.fori_loop(0, tiles, write_step, 0)

    def to_out(flow, base, final, tile):
        cols = pl.ds(pl.multiple_of(tile * width, width), width)
        return pltpu.make_async_copy(final.at[tile], out_ref.at[base : base + half, cols], out_sem.at[flow, tile])

    def final_step(step, carry):
        for flow, base, place, _, back, _, _, final in flows:
            tile = step - lag * (last - place)

            @pl.when((tile >= 0) & (tile < tiles))
            def _():
                @pl.when(place < last)
                def _():
                    send(flow, final, final, fin_send, fin_recv, tile, back).wait_recv()

                    @pl.when(place > 0)
                    def _():
                        send(flow, final, final, fin_send, fin_recv, tile, back).start()

                to_out(flow, base, final, tile).start()

        return carry

    lax.fori_loop(0, tiles + lag * last, final_step, 0)

    def drain_step(tile, carry):
        for flow, base, place, ahead, back, outgoing, incoming, final in flows:
            @pl.when(place < last)
            def _():
                send(flow, outgoing, incoming, sum_send, sum_recv, tile, ahead).wait_send()

            @pl.when(place > 0)
            def _():
                send(flow, final, final, fin_send, fin_recv, tile, back).wait_send()

            to_out(flow, base, final, tile).wait()

        return carry

    lax.fori_loop(0, tiles, drain_step, 0)


def tail(size, attn_out, w_out, x_own, b_out, ln_gamma, ln_beta):
    rows, d_model = x_own.shape
    depth = attn_out.shape[1]
    width = max(128, d_model // 24)
    tiles = d_model // width
    half = rows // 2
    vmem = pl.BlockSpec(memory_space=pltpu.VMEM)
    hbm = pl.BlockSpec(memory_space=pl.ANY)
    row = lambda v: v.astype(jnp.float32)[None]
    strip = pltpu.VMEM((tiles, half, width), jnp.bfloat16)
    return pl.pallas_call(
        functools.partial(tail_kernel, size, 2),
        out_shape=jax.ShapeDtypeStruct((rows, d_model), jnp.bfloat16),
        in_specs=[vmem, hbm, hbm, vmem, vmem, vmem],
        out_specs=hbm,
        scratch_shapes=[
            pltpu.VMEM((tiles, rows, width), jnp.float32),
            pltpu.VMEM((2, depth, width), jnp.bfloat16),
            pltpu.VMEM((rows, d_model), jnp.bfloat16),
            strip, strip, strip, strip, strip, strip,
            pltpu.SemaphoreType.DMA((2,)),
            pltpu.SemaphoreType.DMA,
            pltpu.SemaphoreType.DMA((2, tiles)),
            pltpu.SemaphoreType.DMA((2, tiles)),
            pltpu.SemaphoreType.DMA((2, tiles)),
            pltpu.SemaphoreType.DMA((2, tiles)),
            pltpu.SemaphoreType.DMA((2, tiles)),
        ],
        compiler_params=pltpu.CompilerParams(
            collective_id=0, has_side_effects=True, vmem_limit_bytes=VMEM_LIMIT
        ),
        cost_estimate=pl.CostEstimate(
            flops=2 * rows * depth * d_model, bytes_accessed=2 * depth * d_model, transcendentals=0
        ),
        name="tail",
    )(attn_out, w_out, x_own, row(b_out), row(ln_gamma), row(ln_beta))


def solution(mesh):
    cp_size, tp_size = mesh.shape["cp"], mesh.shape["tp"]
    swap_core = [(i, i ^ 1) for i in range(cp_size)]
    swap_chip = [(i, i ^ 2) for i in range(cp_size)]

    def device_body(x_loc, prefix_len, valid_len, w_qkv, b_qkv, w_out, b_out, ln_gamma, ln_beta):
        batch, piece, d_model = x_loc.shape
        _, _, heads, head_dim = w_qkv.shape
        rows, half_width = batch * piece, heads * head_dim // 2
        depth = min(512, d_model)
        cp_index = lax.axis_index("cp")
        core_index = lax.rem(cp_index, 2)
        core = core_index.astype(jnp.int32).reshape(1)
        near, far = cp_index ^ 1, cp_index ^ 2
        x_own = x_loc.reshape(rows, d_model)
        x_other = lax.ppermute(x_own, "cp", swap_core)
        w_grouped = w_qkv.reshape(d_model, 3, heads // HEAD_GROUP, HEAD_GROUP, head_dim)
        bias = b_qkv.reshape(3, heads * head_dim).astype(jnp.float32)
        spread = jnp.arange(piece)
        positions = jnp.concatenate([cp_index * piece + spread] * batch + [near * piece + spread] * batch)
        cos_tab, sin_tab = rope_tables(positions, head_dim)

        def run(which, after):
            bias_row = jnp.broadcast_to(bias[which][None], (8, heads * head_dim))
            if after is not None:
                bias_row, _ = lax.optimization_barrier((bias_row, after))
            return project(which, core, x_own, x_other, w_grouped, bias_row, cos_tab, sin_tab, depth)

        def gather_heads(own, received):
            low = jnp.where(core_index == 0, own, received)
            high = jnp.where(core_index == 0, received, own)
            return jnp.concatenate([low, high], axis=1)

        keys = run(1, None)
        keys_far = lax.ppermute(keys, "cp", swap_chip)
        keys_back = lax.ppermute(keys[rows:], "cp", swap_core)
        values = run(2, keys)
        values_far = lax.ppermute(values, "cp", swap_chip)
        values_back = lax.ppermute(values[rows:], "cp", swap_core)
        queries = run(0, values)
        k_cache = gather_heads(keys[:rows], keys_back).reshape(batch, piece, heads, head_dim)
        v_cache = gather_heads(values[:rows], values_back).reshape(batch, piece, heads, head_dim)

        info = jnp.concatenate([jnp.stack([cp_index, near, far, far ^ 1]).astype(jnp.int32), prefix_len, valid_len])
        mixed = attend(info, queries, keys, values, keys_far, values_far, batch, head_dim)
        mixed_back = lax.ppermute(mixed[rows:], "cp", swap_core)
        attn_out = gather_heads(mixed[:rows], mixed_back)
        out = tail(tp_size, attn_out, w_out.reshape(2 * half_width, d_model), x_own, b_out, ln_gamma, ln_beta)
        return out.reshape(x_loc.shape), k_cache, v_cache

    return jax.shard_map(
        device_body,
        mesh=mesh,
        in_specs=(
            P("dp", "cp", None),
            P("dp"),
            P("dp"),
            P(None, None, "tp", None),
            P(None, "tp", None),
            P("tp", None, None),
            P(None),
            P(None),
            P(None),
        ),
        out_specs=(P("dp", "cp", None), P("dp", "cp", "tp", None), P("dp", "cp", "tp", None)),
        check_vma=False,
    )
```
